256 devices in a mesh: blk: 8 (over x_hi, y), tok: 32 (over x_lo, z, core).
Axes of the slice: x: 4 (x_hi: 2, x_lo: 2; x = x_hi * 2 + x_lo), y: 4, z: 8, core: 2. Of those that a mesh axis runs over, the one named last changes fastest.
Arguments:
- states: bfloat16 [1024, 3584], P('tok'), may hold values from -30 to 30
- head: bfloat16 [3584, 262144], P(None, ('blk', 'tok')), may hold values from -0.2 to 0.2
- targets: int32 [1024], P('tok'), may hold values from 0 to 262143
- ref_loss: float32 [1024], P('tok'), may hold values from 0 to 8
- seq_ids: int32 [1024], P('tok'), may hold values from 0 to 511, never falling along the last dimension, each value on 1 to 4 neighbouring positions
Outputs:
- excess: float32 [1024], P('tok')
- seq_score: float32 [512], replicated
The draws below stay inside these ranges and needn't reach their ends.
Inputs may be any that keep to these rules, and one draw needn't show every extreme that they name: `seq_ids`: sequence numbers never fall along the tokens; every number from 0 to 511 occurs, on 1 to 4 consecutive tokens.
All inputs are finite; a program needn't handle non-finite values.
Results may differ from the reference program's by a relative error of at most 0.0003.
Values may be sent and summed in bfloat16 or wider, within the bound.
No kernel may reach another device: no remote copies, remote signals or barrier semaphores. Data moves between devices by JAX's collectives and lax.ppermute only.
A program may use at most 64 MiB of HBM per device.

```python
import math
import jax
import jax.numpy as jnp
import numpy as np
from jax import lax

D = 3584
VOCAB = 262144
TOKENS = 1024
SEQS = 512


def joint_draw(key):
    keys = jax.random.split(jax.random.fold_in(key, 7), 4)
    col_scale = jnp.exp(jax.random.uniform(keys[1], (VOCAB,), jnp.float32, math.log(0.5), math.log(2.0)))
    head = jax.random.normal(keys[0], (D, VOCAB), jnp.float32) / math.sqrt(D) * col_scale[None, :]
    head = jnp.clip(head, -0.19921875, 0.19921875)
    base = jax.random.normal(keys[2], (TOKENS, D), jnp.float32)
    row_scale = jnp.exp(jax.random.uniform(keys[3], (TOKENS, 1), jnp.float32, 0.0, math.log(2.0)))
    states = 3.0 * base * row_scale
    states = jnp.clip(states, -30.0, 30.0)
    return (states, head)


def draw_states(key, part):
    return joint_draw(key)[0].astype(jnp.bfloat16)


def draw_head(key, part):
    return joint_draw(key)[1].astype(jnp.bfloat16)


def plant(array, key, smallest, largest):
    spot = [jax.random.randint(jax.random.fold_in(key, axis), (), 0, length) for axis, length in enumerate(array.shape)]
    longest = array.shape.index(max(array.shape))
    neighbour = spot[:longest] + [(spot[longest] + 1) % array.shape[longest]] + spot[longest + 1:]
    return array.at[tuple(spot)].set(smallest).at[tuple(neighbour)].set(largest)


def block_levels(stream_key, extent, cuts, least, largest):
    loudness, own = 1.0, jax.random.fold_in(stream_key, 6)
    for axis_at, parts in cuts:
        draws = jnp.exp(jax.random.uniform(jax.random.fold_in(own, axis_at), (parts,), jnp.float32, least / len(cuts), largest / len(cuts)))
        loudness = loudness * jnp.repeat(draws, extent[axis_at] // parts).reshape([-1 if axis == axis_at else 1 for axis in range(len(extent))])
    return loudness


def split_up(count, total, most, lean):
    portions = [(1 << 20) // math.isqrt(rank ** lean) + 1 for rank in range(2, count + 1)]
    spare, holding = total - most - (count - 1), [1] * (count - 1)
    while spare > 0:
        free = [i for i in range(count - 1) if holding[i] < most]
        mass, remaining = sum([portions[i] for i in free]), spare
        for i in free:
            extra = min(most - holding[i], max(1, remaining * portions[i] // mass), spare)
            holding[i] = holding[i] + extra
            spare = spare - extra
    return np.array([most] + holding)


def ragged(key, count, total, reach, slope):
    if count == 2:
        one = jax.random.randint(key, (), max(1, total - reach), min(reach, total - 1) + 1)
        return jnp.stack([one, total - one])
    lengths = jnp.asarray(split_up(count, total, reach, slope), jnp.int32)
    pairs = (count - 1) // 2
    source_of, sink = lengths[1:1 + 2 * pairs:2], lengths[2:2 + 2 * pairs:2]
    margin = jnp.minimum(source_of - 1, reach - sink)
    shifted = jax.random.randint(jax.random.fold_in(key, 1), (pairs,), 0, 1 << 20) % (margin + 1)
    lengths = lengths.at[1:1 + 2 * pairs:2].set(source_of - shifted).at[2:2 + 2 * pairs:2].set(sink + shifted)
    return lengths[jax.random.permutation(jax.random.fold_in(key, 2), count)]


def setup_inputs(seed: int = 0) -> dict:
    key_of = jax.random.split(jax.random.key(seed), 6)
    return {
        "states": draw_states(jax.random.fold_in(key_of[5], 71), 0),
        "head": draw_head(jax.random.fold_in(key_of[5], 71), 0),
        "targets": plant(jax.random.randint(key_of[2], (TOKENS,), 0, VOCAB), jax.random.fold_in(key_of[2], 1), 0, VOCAB - 1).astype(jnp.int32),
        "ref_loss": jnp.clip(8.0 * jax.random.uniform(key_of[3], (TOKENS,), jnp.float32) ** block_levels(key_of[3], (TOKENS,), ((0, 32),), -0.2, 0.2), 0.0, 8.0),
        "seq_ids": jnp.searchsorted(jnp.cumsum(ragged(key_of[4], SEQS, TOKENS, 4, 2)), jnp.arange(TOKENS), side="right").astype(jnp.int32),
    }


def reference(states, head, targets, ref_loss, seq_ids):
    group = min(256, TOKENS)
    while TOKENS % group != 0:
        group = group // 2
    blocks = TOKENS // group

    def score(operands):
        token_rows, target_ids = operands
        logits = jnp.dot(token_rows, head, preferred_element_type=jnp.float32)
        highest = jnp.max(logits, axis=1)
        log_total = highest + jnp.log(jnp.sum(jnp.exp(logits - highest[:, None]), axis=1))
        picked = jnp.take_along_axis(logits, target_ids[:, None].astype(jnp.int32), axis=1)[:, 0]
        return log_total - picked

    values = lax.map(score, (states.reshape(blocks, group, D), targets.reshape(blocks, group)))
    excess = values.reshape(TOKENS) - ref_loss
    totals = jax.ops.segment_sum(excess, seq_ids, num_segments=SEQS)
    counts = jax.ops.segment_sum(jnp.ones((TOKENS,), jnp.float32), seq_ids, num_segments=SEQS)
    return excess, totals / counts
```

```python
import jax
import jax.numpy as jnp
from jax import lax
from jax.sharding import Mesh
from jax.sharding import PartitionSpec as P


TOK = ("xl", "z", "c")
BLK_TOK = ("xh", "y", "xl", "z", "c")
X = ("xh", "xl")
PLANE = ("xh", "xl", "y")


def hop(value, axis, step):
    n = lax.axis_size(axis)
    return lax.ppermute(value, axis, [(i, (i + step) % n) for i in range(n)])


def from_everyone(value, axis):
    n = lax.axis_size(axis)
    return lax.all_to_all(
        jnp.broadcast_to(value[None], (n, *value.shape)), axis, 0, 0, tiled=True
    )


def chunk_stats(rows, heads, target_ids, first_cols):
    logits = [jnp.dot(rows, h, preferred_element_type=jnp.float32) for h in heads]
    highest = jnp.maximum(*[jnp.max(l, axis=1) for l in logits])
    scaled = sum(jnp.sum(jnp.exp(l - highest[:, None]), axis=1) for l in logits)
    picked = 0.0
    for l, first in zip(logits, first_cols):
        columns = first + lax.broadcasted_iota(jnp.int32, l.shape, 1)
        picked += jnp.sum(jnp.where(columns == target_ids[:, None], l, 0.0), axis=1)
    return highest + jnp.log(scaled), picked


def lse_over(parts):
    highest = jnp.max(parts, axis=0)
    return highest + jnp.log(jnp.sum(jnp.exp(parts - highest[None]), axis=0))


def on_device(states, head, targets, ref_loss, seq_ids):
    xl, z, c = (lax.axis_index(a) for a in TOK)
    nz = lax.axis_size("z")
    half = nz // 2
    local = states.shape[0]
    width = head.shape[1]
    partner_head = hop(head, "c", 1)
    own, far = {0: states}, {}
    up = down = states
    far[0] = hop(states, X, 1)
    for d in range(1, half):
        up, down = hop(up, "z", 1), hop(down, "z", -1)
        own[-d], own[d] = up, down
        far[-d], far[d] = hop(up, X, 1), hop(down, X, -1)
    mid = local // 2
    top, bottom = hop(up[:mid], "z", 1), hop(down[mid:], "z", -1)
    own[half] = jnp.concatenate([top, bottom])
    far[half] = jnp.concatenate([hop(top, X, 1), hop(bottom, X, -1)])

    ids = from_everyone(targets[None], ("xl", "z")).reshape(2, nz, local)
    ids = jnp.concatenate([ids, ids], axis=1)
    seen = {}
    start = lax.rem(z + nz - (half - 1), nz)
    ids = lax.dynamic_slice_in_dim(ids, start, nz, axis=1)
    ids = jnp.where(xl == 0, ids, ids[::-1])
    for d in range(1 - half, half + 1):
        seen[0, d], seen[1, d] = ids[0, d + half - 1], ids[1, d + half - 1]

    blk = lax.axis_index(("xh", "y"))
    block = blk * lax.axis_size(TOK) + (xl * nz + z) * 2
    first_cols = ((block + c) * width, (block + 1 - c) * width)
    groups = [
        [(0, 0), (0, -1), (0, 1), (0, -2), (0, 2), (1, 0), (1, -1), (1, 1)],
        [(0, -3), (0, 3), (1, -2), (1, 2), (1, -3), (1, 3)],
        [(0, 4), (1, 4)],
    ]
    lse, picked = {}, {}
    for group in groups:
        rows = jnp.concatenate([(far if o else own)[d] for o, d in group])
        wanted = jnp.concatenate([seen[k] for k in group])
        a, b = chunk_stats(rows, (head, partner_head), wanted, first_cols)
        for k, key in enumerate(group):
            lse[key] = a[k * local : (k + 1) * local]
            picked[key] = b[k * local : (k + 1) * local]
    picked[0, 0] = picked[0, 0] + jnp.where(blk == 0, ref_loss, 0.0)
    order = range(1 - half, half + 1)
    stats = jnp.stack(
        [
            jnp.stack([jnp.stack([part[o, d] for d in order]) for o in range(2)])
            for part in (lse, picked)
        ]
    )
    stats = jnp.concatenate([stats, stats], axis=2)
    stats = lax.dynamic_slice_in_dim(stats, lax.rem(half - 1 - z + nz, nz), nz, axis=2)
    stats = jnp.where(xl == 0, stats, stats[:, ::-1])
    stats = stats.reshape(2, -1)

    for axes in (PLANE, ("z",)):
        parts = from_everyone(stats, axes)
        stats = jnp.stack([lse_over(parts[:, 0]), jnp.sum(parts[:, 1], axis=0)])
    all_excess = stats[0] - stats[1]
    excess = lax.dynamic_slice_in_dim(all_excess, (xl * nz + z) * local, local)

    seqs = from_everyone(seq_ids[None], ("xl", "z")).reshape(-1)
    count = all_excess.shape[0]
    member = (seqs[:, None] == lax.iota(jnp.int32, count)[None, :]).astype(jnp.float32)
    totals = jnp.dot(all_excess, member, precision=lax.Precision.HIGHEST)
    counts = jnp.sum(member, axis=0)
    sums = jnp.stack([totals, counts])
    sums = sums + hop(sums, "c", 1)
    return excess, sums[0] / sums[1]


def solution(mesh):
    torus = Mesh(mesh.devices.reshape(2, 4, 2, 8, 2), BLK_TOK)
    return jax.shard_map(
        on_device,
        mesh=torus,
        in_specs=(P(TOK, None), P(None, BLK_TOK), P(TOK), P(TOK), P(TOK)),
        out_specs=(P(TOK), P()),
        check_vma=False,
    )
```

```python
import functools

import jax
import jax.numpy as jnp
from jax import lax
from jax.experimental import pallas as pl
from jax.experimental.pallas import tpu as pltpu
from jax.sharding import Mesh
from jax.sharding import PartitionSpec as P


TOK = ("xl", "z", "c")
BLK_TOK = ("xh", "y", "xl", "z", "c")
X = ("xh", "xl")
PLANE = ("xh", "xl", "y")
LANES = 128
TILE = 256
VMEM_BYTES = 67043328

VMEM = pl.BlockSpec(memory_space=pltpu.VMEM)
SMEM = pl.BlockSpec(memory_space=pltpu.SMEM)
HBM = pl.BlockSpec(memory_space=pltpu.HBM)


def hop(value, axis, step):
    n = lax.axis_size(axis)
    return lax.ppermute(value, axis, [(i, (i + step) % n) for i in range(n)])


def exchange(copies, axis):
    return lax.all_to_all(copies, axis, 0, 0, tiled=True)


def tag_kernel(states_in, targets_in, loss_in, seq_in, out_ref, targets_ref, loss_ref, seq_ref, sems):
    local, depth = states_in.shape
    pairs = (
        (targets_in, targets_ref),
        (loss_in, loss_ref),
        (seq_in, seq_ref),
        (states_in, out_ref.at[:, pl.ds(0, depth)]),
    )
    copies = [pltpu.make_async_copy(a, b, sems.at[k]) for k, (a, b) in enumerate(pairs)]
    for copy in copies:
        copy.start()
    for copy in copies[:3]:
        copy.wait()
    target, seq, loss = targets_ref[...], seq_ref[...], loss_ref[...]
    high = loss.astype(jnp.bfloat16).astype(jnp.float32)
    middle = (loss - high).astype(jnp.bfloat16).astype(jnp.float32)
    tags = [target >> 16, (target >> 8) & 255, target & 255, seq >> 8, seq & 255]
    tags = [t.astype(jnp.float32) for t in tags] + [high, middle, loss - high - middle]
    row = lax.broadcasted_iota(jnp.int32, (LANES, local), 0)
    columns = jnp.zeros((LANES, local), jnp.float32)
    for k, tag in enumerate(tags):
        columns = jnp.where(row == k, tag, columns)
    columns = jnp.concatenate([columns, jnp.zeros((LANES, LANES - local), jnp.float32)], axis=1)
    out_ref[:, depth:] = columns.T[:local].astype(jnp.bfloat16)
    copies[3].wait()


def score_kernel(index_ref, a_ref, b_ref, *refs):
    *blocks, stats_ref, meta_ref, x_ref, tiles, logits, peak, sems = refs
    rows, depth = x_ref.shape[0], a_ref.shape[0]
    per_head = a_ref.shape[1] // TILE
    count = 2 * per_head
    for j in range(count):
        source = (a_ref, b_ref)[j // per_head].at[:, pl.ds(j % per_head * TILE, TILE)]
        pltpu.make_async_copy(source, tiles.at[j], sems.at[j]).start()
    peak[...] = jnp.full(peak.shape, -jnp.inf, jnp.float32)
    for k, block in enumerate(blocks):
        place = pl.multiple_of(index_ref[3 + k], 16)
        x_ref[pl.ds(place, block.shape[0]), :] = block[...]

    def multiply(j, carry):
        pltpu.make_async_copy(a_ref.at[:, pl.ds(0, TILE)], tiles.at[j], sems.at[j]).wait()
        part = jnp.dot(x_ref[:, :depth], tiles[j], preferred_element_type=jnp.float32)
        logits[j] = part
        top = peak[...]
        for h in range(TILE // LANES):
            top = jnp.maximum(top, part[:, h * LANES : (h + 1) * LANES])
        peak[...] = top
        return carry

    lax.fori_loop(0, count, multiply, 0)

    lane = lax.broadcasted_iota(jnp.int32, (1, LANES), 1).astype(jnp.float32)

    def read(tags, scales):
        weight = jnp.zeros(lane.shape, jnp.float32)
        for k, scale in scales:
            weight = jnp.where(lane == k, scale, weight)
        return tags * weight

    for r in range(rows // LANES):
        span = pl.ds(r * LANES, LANES)
        tags = x_ref[span, depth : depth + LANES].astype(jnp.float32)
        target = jnp.sum(read(tags, ((0, 65536.0), (1, 256.0), (2, 1.0))), axis=1, keepdims=True)
        top = peak[span, :]
        highest = jnp.max(top, axis=1, keepdims=True)
        scaled = jnp.zeros((LANES, LANES), jnp.float32)
        picked = jnp.zeros((LANES, LANES), jnp.float32)
        for j in range(count):
            for h in range(TILE // LANES):
                part = logits[j, span, h * LANES : (h + 1) * LANES]
                scaled += jnp.exp(part - highest)
                first = index_ref[j // per_head] + (j % per_head * TILE + h * LANES)
                picked += jnp.where(lane == target - first.astype(jnp.float32), part, 0.0)
        lse = jnp.max(top.T, axis=0, keepdims=True) + jnp.log(
            jnp.sum(scaled.T, axis=0, keepdims=True)
        )
        chosen = jnp.sum(picked.T, axis=0, keepdims=True)
        for k in range(stats_ref.shape[0]):
            stats_ref[k, :, r * LANES : (r + 1) * LANES] = lse
            stats_ref[k, :, rows + r * LANES : rows + (r + 1) * LANES] = chosen
        seq = jnp.sum(read(tags, ((3, 256.0), (4, 1.0))).T, axis=0, keepdims=True)
        parts = tags.T
        meta_ref[0:1, r * LANES : (r + 1) * LANES] = seq
        meta_ref[1:2, r * LANES : (r + 1) * LANES] = parts[5:6] + parts[6:7] + parts[7:8]


def merged(parts_ref):
    n, _, width = parts_ref.shape
    rows = width // 2
    lses = [parts_ref[k, :, :rows] for k in range(n)]
    highest = functools.reduce(jnp.maximum, lses)
    lse = highest + jnp.log(sum(jnp.exp(l - highest) for l in lses))
    return lse, sum(parts_ref[k, :, rows:] for k in range(n))


def merge_kernel(parts_ref, out_ref):
    lse, picked = merged(parts_ref)
    rows = lse.shape[1]
    for k in range(out_ref.shape[0]):
        out_ref[k, :, :rows] = lse
        out_ref[k, :, rows:] = picked


def finish_kernel(index_ref, parts_ref, meta_ref, own_ref, sums_ref):
    lse, picked = merged(parts_ref)
    excess = lse - picked - meta_ref[1:2, :]
    rows, count = excess.shape[1], sums_ref.shape[1]
    own_ref[...] = pltpu.roll(excess, lax.rem(rows - index_ref[2], rows), 1)[:, :LANES]
    seq = lax.broadcasted_iota(jnp.int32, (count, rows), 0).astype(jnp.float32)
    member = (seq == meta_ref[0:1, :]).astype(jnp.float32)
    left = jnp.concatenate([excess, jnp.ones_like(excess)], axis=0)
    left = jnp.concatenate([left, jnp.zeros((6, rows), jnp.float32)], axis=0)
    sums = lax.dot_general(
        left, member, (((1,), (1,)), ((), ())),
        precision=lax.Precision.HIGHEST, preferred_element_type=jnp.float32,
    )
    sums_ref[...] = sums[0:2]


def ratio_kernel(mine_ref, other_ref, out_ref):
    total = mine_ref[...] + other_ref[...]
    out_ref[...] = total[0:1] / total[1:2]


def on_device(states, head, targets, ref_loss, seq_ids):
    xl, z, c = (lax.axis_index(a) for a in TOK)
    nz = lax.axis_size("z")
    half = nz // 2
    local = states.shape[0]
    depth, width = head.shape
    partner_head = hop(head, "c", 1)
    tagged = pl.pallas_call(
        tag_kernel,
        out_shape=jax.ShapeDtypeStruct((local, depth + LANES), jnp.bfloat16),
        in_specs=[HBM] * 4,
        out_specs=VMEM,
        scratch_shapes=[
            pltpu.VMEM((1, local), jnp.int32),
            pltpu.VMEM((1, local), jnp.float32),
            pltpu.VMEM((1, local), jnp.int32),
            pltpu.SemaphoreType.DMA((4,)),
        ],
        compiler_params=pltpu.CompilerParams(
            vmem_limit_bytes=VMEM_BYTES - 3 * local * (depth + LANES)
        ),
        name="tag",
    )(states, targets[None], ref_loss[None], seq_ids[None])

    up = down = tagged
    mid = local // 2
    blocks, where = [tagged], [(0, 0, 0)]
    for d in range(1, half + 1):
        skip = 0
        if d == half:
            up, down, skip = up[:mid], down[mid:], mid
        up = hop(up, "z", 1)
        down = hop(down, "z", -1)
        if d == 1:
            blocks.append(hop(tagged, X, 1))
            where.append((0, 1, 0))
        far_up = hop(up, X, 1)
        far_down = hop(down, X, -1)
        blocks += [up, down, far_up, far_down]
        where += [(-d, 0, 0), (d, 0, skip), (-d, 1, 0), (d, 1, skip)]

    block = lax.axis_index(("xh", "y")) * lax.axis_size(TOK) + (xl * nz + z) * 2
    distance, other, skip = jnp.asarray([(0, 0, 0)] * 3 + where, jnp.int32).T
    k = lax.iota(jnp.int32, distance.shape[0])
    index = ((xl ^ other) * nz + ((z + distance) & (nz - 1))) * local + skip
    index = jnp.where(k == 0, (block + c) * width, index)
    index = jnp.where(k == 1, (block + 1 - c) * width, index)
    tokens = 2 * nz * local
    plane = lax.axis_size(PLANE)
    count = 2 * width // TILE
    stats, meta = pl.pallas_call(
        score_kernel,
        out_shape=(
            jax.ShapeDtypeStruct((nz, 1, 2 * tokens), jnp.float32),
            jax.ShapeDtypeStruct((2, tokens), jnp.float32),
        ),
        in_specs=[SMEM, HBM, HBM] + [VMEM] * len(blocks),
        out_specs=(VMEM, VMEM),
        scratch_shapes=[
            pltpu.VMEM((tokens, depth + LANES), jnp.bfloat16),
            pltpu.VMEM((count, depth, TILE), jnp.bfloat16),
            pltpu.VMEM((count, tokens, TILE), jnp.float32),
            pltpu.VMEM((tokens, LANES), jnp.float32),
            pltpu.SemaphoreType.DMA((count,)),
        ],
        compiler_params=pltpu.CompilerParams(vmem_limit_bytes=48 << 20),
        cost_estimate=pl.CostEstimate(
            flops=4 * tokens * depth * width, bytes_accessed=4 * depth * width, transcendentals=0
        ),
        name="score",
    )(index, head, partner_head, *blocks)
    stats = pl.pallas_call(
        merge_kernel,
        out_shape=jax.ShapeDtypeStruct((plane, 1, 2 * tokens), jnp.float32),
        in_specs=[VMEM],
        out_specs=VMEM,
        compiler_params=pltpu.CompilerParams(vmem_limit_bytes=2 << 20),
        name="merge",
    )(exchange(stats, "z"))
    own, sums = pl.pallas_call(
        finish_kernel,
        out_shape=(
            jax.ShapeDtypeStruct((1, LANES), jnp.float32),
            jax.ShapeDtypeStruct((2, tokens), jnp.float32),
        ),
        in_specs=[SMEM, VMEM, VMEM],
        out_specs=(VMEM, VMEM),
        compiler_params=pltpu.CompilerParams(vmem_limit_bytes=4 << 20),
        name="finish",
    )(index, exchange(stats, PLANE), meta)
    ratio = pl.pallas_call(
        ratio_kernel,
        out_shape=jax.ShapeDtypeStruct((1, tokens), jnp.float32),
        in_specs=[VMEM, VMEM],
        out_specs=VMEM,
        compiler_params=pltpu.CompilerParams(vmem_limit_bytes=2 << 20),
        name="ratio",
    )(sums, hop(sums, "c", 1))
    return own[0, :local], ratio[0]


def solution(mesh):
    torus = Mesh(mesh.devices.reshape(2, 4, 2, 8, 2), BLK_TOK)
    return jax.shard_map(
        on_device,
        mesh=torus,
        in_specs=(P(TOK, None), P(None, BLK_TOK), P(TOK), P(TOK), P(TOK)),
        out_specs=(P(TOK), P()),
        check_vma=False,
    )
```

```python
import functools

import jax
import jax.numpy as jnp
from jax import lax
from jax.experimental import pallas as pl
from jax.experimental.pallas import tpu as pltpu
from jax.sharding import Mesh
from jax.sharding import PartitionSpec as P


TOK = ("xl", "z", "c")
BLK_TOK = ("xh", "y", "xl", "z", "c")
X = ("xh", "xl")
PLANE = ("xh", "xl", "y")
LANES = 128
TILE = 256
VMEM_BYTES = 67043328
HEADER = 5

VMEM = pl.BlockSpec(memory_space=pltpu.VMEM)
SMEM = pl.BlockSpec(memory_space=pltpu.SMEM)
HBM = pl.BlockSpec(memory_space=pltpu.HBM)


def hop(value, axis, step):
    n = lax.axis_size(axis)
    return lax.ppermute(value, axis, [(i, (i + step) % n) for i in range(n)])


def exchange(copies, axis):
    return lax.all_to_all(copies, axis, 0, 0, tiled=True)


def tag_kernel(states_in, targets_in, loss_in, seq_in, out_ref, targets_ref, loss_ref, seq_ref, sems):
    local, depth = states_in.shape
    pairs = (
        (targets_in, targets_ref),
        (loss_in, loss_ref),
        (seq_in, seq_ref),
        (states_in, out_ref.at[:, pl.ds(0, depth)]),
    )
    copies = [pltpu.make_async_copy(a, b, sems.at[k]) for k, (a, b) in enumerate(pairs)]
    for copy in copies:
        copy.start()
    for copy in copies[:3]:
        copy.wait()
    target, seq, loss = targets_ref[...], seq_ref[...], loss_ref[...]
    high = loss.astype(jnp.bfloat16).astype(jnp.float32)
    middle = (loss - high).astype(jnp.bfloat16).astype(jnp.float32)
    tags = [target >> 16, (target >> 8) & 255, target & 255, seq >> 8, seq & 255]
    tags = [t.astype(jnp.float32) for t in tags] + [high, middle, loss - high - middle]
    row = lax.broadcasted_iota(jnp.int32, (LANES, local), 0)
    columns = jnp.zeros((LANES, local), jnp.float32)
    for k, tag in enumerate(tags):
        columns = jnp.where(row == k, tag, columns)
    columns = jnp.concatenate([columns, jnp.zeros((LANES, LANES - local), jnp.float32)], axis=1)
    out_ref[:, depth:] = columns.T[:local].astype(jnp.bfloat16)
    copies[3].wait()


def score_kernel(index_ref, a_ref, b_ref, *refs):
    *blocks, stats_ref, meta_ref, x_ref, tiles, logits, peak, sems = refs
    rows, depth = x_ref.shape[0], a_ref.shape[0]
    per_head = a_ref.shape[1] // TILE
    count = 2 * per_head
    for j in range(count):
        source = (a_ref, b_ref)[j // per_head].at[:, pl.ds(j % per_head * TILE, TILE)]
        pltpu.make_async_copy(source, tiles.at[j], sems.at[j]).start()
    peak[...] = jnp.full(peak.shape, -jnp.inf, jnp.float32)

    def take(some):
        for k in some:
            place = pl.multiple_of(index_ref[HEADER + k], blocks[k].shape[0])
            x_ref[pl.ds(place, blocks[k].shape[0]), :] = blocks[k][...]

    first, last = range(4), range(len(blocks) - 4, len(blocks))
    take(range(4, len(blocks) - 4))
    pl.when(index_ref[2] == 0)(lambda: take(first))
    pl.when(index_ref[2] != 0)(lambda: take(last))

    def multiply(j, carry):
        pltpu.make_async_copy(a_ref.at[:, pl.ds(0, TILE)], tiles.at[j], sems.at[j]).wait()
        part = jnp.dot(x_ref[:, :depth], tiles[j], preferred_element_type=jnp.float32)
        logits[j] = part
        top = peak[...]
        for h in range(TILE // LANES):
            top = jnp.maximum(top, part[:, h * LANES : (h + 1) * LANES])
        peak[...] = top
        return carry

    lax.fori_loop(0, count, multiply, 0)

    lane = lax.broadcasted_iota(jnp.int32, (1, LANES), 1).astype(jnp.float32)

    def read(tags, scales):
        weight = jnp.zeros(lane.shape, jnp.float32)
        for k, scale in scales:
            weight = jnp.where(lane == k, scale, weight)
        return tags * weight

    for r in range(rows // LANES):
        span = pl.ds(r * LANES, LANES)
        tags = x_ref[span, depth : depth + LANES].astype(jnp.float32)
        target = jnp.sum(read(tags, ((0, 65536.0), (1, 256.0), (2, 1.0))), axis=1, keepdims=True)
        top = peak[span, :]
        highest = jnp.max(top, axis=1, keepdims=True)
        scaled = jnp.zeros((LANES, LANES), jnp.float32)
        picked = jnp.zeros((LANES, LANES), jnp.float32)
        for j in range(count):
            for h in range(TILE // LANES):
                part = logits[j, span, h * LANES : (h + 1) * LANES]
                scaled += jnp.exp(part - highest)
                column = index_ref[j // per_head] + (j % per_head * TILE + h * LANES)
                picked += jnp.where(lane == target - column.astype(jnp.float32), part, 0.0)
        lse = jnp.max(top.T, axis=0, keepdims=True) + jnp.log(
            jnp.sum(scaled.T, axis=0, keepdims=True)
        )
        chosen = jnp.sum(picked.T, axis=0, keepdims=True)
        for k in range(stats_ref.shape[0]):
            stats_ref[k, :, r * LANES : (r + 1) * LANES] = lse
            stats_ref[k, :, rows + r * LANES : rows + (r + 1) * LANES] = chosen
        seq = jnp.sum(read(tags, ((3, 256.0), (4, 1.0))).T, axis=0, keepdims=True)
        parts = tags.T
        meta_ref[0:1, r * LANES : (r + 1) * LANES] = seq
        meta_ref[1:2, r * LANES : (r + 1) * LANES] = parts[5:6] + parts[6:7] + parts[7:8]


def merged(parts_ref):
    n, _, width = parts_ref.shape
    rows = width // 2
    lses = [parts_ref[k, :, :rows] for k in range(n)]
    highest = functools.reduce(jnp.maximum, lses)
    lse = highest + jnp.log(sum(jnp.exp(l - highest) for l in lses))
    return lse, sum(parts_ref[k, :, rows:] for k in range(n))


def merge_kernel(parts_ref, meta_ref, out_ref):
    lse, picked = merged(parts_ref)
    rows = lse.shape[1]
    for k in range(out_ref.shape[0]):
        for i, value in enumerate((lse, picked, meta_ref[0:1, :], meta_ref[1:2, :])):
            out_ref[k, :, i * rows : (i + 1) * rows] = value


def held(z, c, nz):
    half = nz // 2
    return {(z - s if c == 0 else z + 1 + s) % nz for s in range(half)}


def finish_kernel(index_ref, parts_ref, own_ref, score_ref, *, nz, span):
    rows, count, half = parts_ref.shape[2] // 4, score_ref.shape[1], nz // 2
    lane = lax.broadcasted_iota(jnp.int32, (1, rows), 1)
    slot = lax.rem(lax.div(lane, span), half)

    def field(k, i):
        return parts_ref[k, :, i * rows : (i + 1) * rows]

    excesses, sums = [], None
    for low in (True, False):
        lses, picked = [], jnp.zeros((1, rows), jnp.float32)
        seq, loss = jnp.zeros((1, rows), jnp.float32), jnp.zeros((1, rows), jnp.float32)
        for k in range(2 * nz):
            zs = [z for z in held(k // 2, k % 2, nz) if (z < half) == low]
            if not zs:
                continue
            here = functools.reduce(jnp.logical_or, [slot == z % half for z in zs])
            lses.append(jnp.where(here, field(k, 0), -jnp.inf))
            picked += jnp.where(here, field(k, 1), 0.0)
        for z in range(nz):
            if (z < half) == low:
                here = slot == z % half
                seq = jnp.where(here, field(2 * z, 2), seq)
                loss = jnp.where(here, field(2 * z, 3), loss)
        highest = functools.reduce(jnp.maximum, lses)
        lse = highest + jnp.log(sum(jnp.exp(l - highest) for l in lses))
        excess = lse - picked - loss
        excesses.append(excess)
        ids = lax.broadcasted_iota(jnp.int32, (count, rows), 0).astype(jnp.float32)
        member = jnp.where(ids == seq, 1.0, 0.0).astype(jnp.bfloat16)
        high = excess.astype(jnp.bfloat16).astype(jnp.float32)
        middle = (excess - high).astype(jnp.bfloat16).astype(jnp.float32)
        pieces = [high, middle, excess - high - middle, jnp.ones_like(excess)]
        row = lax.broadcasted_iota(jnp.int32, (16, rows), 0)
        left = jnp.zeros((16, rows), jnp.float32)
        for i, piece in enumerate(pieces):
            left = jnp.where(row == i, piece, left)
        part = lax.dot_general(
            left.astype(jnp.bfloat16), member, (((1,), (1,)), ((), ())),
            preferred_element_type=jnp.float32,
        )
        sums = part if sums is None else sums + part
    score_ref[...] = (sums[0:1] + sums[1:2] + sums[2:3]) / sums[3:4]
    mine = jnp.where(index_ref[4] == 0, excesses[0], excesses[1])
    own_ref[...] = pltpu.roll(mine, lax.rem(rows - index_ref[3], rows), 1)[:, :LANES]


def on_device(states, head, targets, ref_loss, seq_ids):
    xl, z, c = (lax.axis_index(a) for a in TOK)
    nz = lax.axis_size("z")
    half = nz // 2
    local = states.shape[0]
    depth, width = head.shape
    tagged = pl.pallas_call(
        tag_kernel,
        out_shape=jax.ShapeDtypeStruct((local, depth + LANES), jnp.bfloat16),
        in_specs=[HBM] * 4,
        out_specs=VMEM,
        scratch_shapes=[
            pltpu.VMEM((1, local), jnp.int32),
            pltpu.VMEM((1, local), jnp.float32),
            pltpu.VMEM((1, local), jnp.int32),
            pltpu.SemaphoreType.DMA((4,)),
        ],
        compiler_params=pltpu.CompilerParams(
            vmem_limit_bytes=VMEM_BYTES - 3 * local * (depth + LANES)
        ),
        name="tag",
    )(states, targets[None], ref_loss[None], seq_ids[None])

    other_half = hop(tagged, "c", 1)

    def along(value, axis, first, second):
        n = lax.axis_size(axis)
        pairs = [(2 * i, (i + 1) % n * 2) for i in range(n)] if first else []
        pairs += [(2 * i + 1, (i - 1) % n * 2 + 1) for i in range(n)] if second else []
        axes = (axis, "c") if isinstance(axis, str) else (*axis, "c")
        return lax.ppermute(value, axes, pairs)

    near = [tagged, other_half]
    blocks, where = [], []
    for s in range(half + 1):
        if s > 0:
            for k in range(2):
                near[k] = along(near[k], "z", s < half, True)
        for k in range(2):
            far = along(near[k], X, s < half, s > 0)
            blocks += [near[k], far]
            where += [(s, 0, k), (s, 1, k)]
    partner_head = hop(head, "c", 1)

    block = lax.axis_index(("xh", "y")) * lax.axis_size(TOK) + (xl * nz + z) * 2
    steps, other, piece = jnp.asarray([(0, 0, 0)] * HEADER + where, jnp.int32).T
    k = lax.iota(jnp.int32, steps.shape[0])
    span = 2 * local
    slot = lax.rem(z + jnp.where(c == 0, nz - steps, steps), half)
    index = ((xl ^ other) * half + slot) * span + (c ^ piece) * local
    fixed = ((block + c) * width, (block + 1 - c) * width, c, (xl * half + z % half) * span + c * local, z // half)
    for i, value in enumerate(fixed):
        index = jnp.where(k == i, value, index)
    tokens = 2 * nz * local
    plane = lax.axis_size(PLANE)
    count = 2 * width // TILE
    stats, meta = pl.pallas_call(
        score_kernel,
        out_shape=(
            jax.ShapeDtypeStruct((plane, 1, 2 * tokens), jnp.float32),
            jax.ShapeDtypeStruct((2, tokens), jnp.float32),
        ),
        in_specs=[SMEM, HBM, HBM] + [VMEM] * len(blocks),
        out_specs=(VMEM, VMEM),
        scratch_shapes=[
            pltpu.VMEM((tokens, depth + LANES), jnp.bfloat16),
            pltpu.VMEM((count, depth, TILE), jnp.bfloat16),
            pltpu.VMEM((count, tokens, TILE), jnp.float32),
            pltpu.VMEM((tokens, LANES), jnp.float32),
            pltpu.SemaphoreType.DMA((count,)),
        ],
        compiler_params=pltpu.CompilerParams(vmem_limit_bytes=45 << 20),
        cost_estimate=pl.CostEstimate(
            flops=4 * tokens * depth * width, bytes_accessed=4 * depth * width, transcendentals=0
        ),
        name="score",
    )(index, head, partner_head, *blocks)
    stats = pl.pallas_call(
        merge_kernel,
        out_shape=jax.ShapeDtypeStruct((2 * nz, 1, 4 * tokens), jnp.float32),
        in_specs=[VMEM, VMEM],
        out_specs=VMEM,
        compiler_params=pltpu.CompilerParams(vmem_limit_bytes=2 << 20),
        name="merge",
    )(exchange(stats, PLANE), meta)
    own, score = pl.pallas_call(
        functools.partial(finish_kernel, nz=nz, span=span),
        out_shape=(
            jax.ShapeDtypeStruct((1, LANES), jnp.float32),
            jax.ShapeDtypeStruct((1, tokens), jnp.float32),
        ),
        in_specs=[SMEM, VMEM],
        out_specs=(VMEM, VMEM),
        compiler_params=pltpu.CompilerParams(vmem_limit_bytes=8 << 20),
        name="finish",
    )(index, exchange(stats, ("z", "c")))
    return own[0, :local], score[0]


def solution(mesh):
    torus = Mesh(mesh.devices.reshape(2, 4, 2, 8, 2), BLK_TOK)
    return jax.shard_map(
        on_device,
        mesh=torus,
        in_specs=(P(TOK, None), P(None, BLK_TOK), P(TOK), P(TOK), P(TOK)),
        out_specs=(P(TOK), P()),
        check_vma=False,
    )
```

```python
import functools

import jax
import jax.numpy as jnp
from jax import lax
from jax.experimental import pallas as pl
from jax.experimental.pallas import tpu as pltpu
from jax.sharding import Mesh
from jax.sharding import PartitionSpec as P


TOK = ("xl", "z", "c")
BLK_TOK = ("xh", "y", "xl", "z", "c")
X = ("xh", "xl")
PLANE = ("xh", "xl", "y")
LANES = 128
TILE = 512
VMEM_BYTES = 67043328
HEADER = 6

VMEM = pl.BlockSpec(memory_space=pltpu.VMEM)
SMEM = pl.BlockSpec(memory_space=pltpu.SMEM)
HBM = pl.BlockSpec(memory_space=pltpu.HBM)


def hop(value, axis, step):
    n = lax.axis_size(axis)
    return lax.ppermute(value, axis, [(i, (i + step) % n) for i in range(n)])


def exchange(copies, axis):
    return lax.all_to_all(copies, axis, 0, 0, tiled=True)


def tag_kernel(states_in, targets_in, loss_in, seq_in, out_ref, targets_ref, loss_ref, seq_ref, sems):
    local, depth = states_in.shape
    pairs = (
        (targets_in, targets_ref),
        (loss_in, loss_ref),
        (seq_in, seq_ref),
        (states_in, out_ref.at[:, pl.ds(0, depth)]),
    )
    copies = [pltpu.make_async_copy(a, b, sems.at[k]) for k, (a, b) in enumerate(pairs)]
    for copy in copies:
        copy.start()
    for copy in copies[:3]:
        copy.wait()
    target, seq, loss = targets_ref[...], seq_ref[...], loss_ref[...]
    high = loss.astype(jnp.bfloat16).astype(jnp.float32)
    middle = (loss - high).astype(jnp.bfloat16).astype(jnp.float32)
    tags = [target >> 16, (target >> 8) & 255, target & 255, seq >> 8, seq & 255]
    tags = [t.astype(jnp.float32) for t in tags] + [high, middle, loss - high - middle]
    row = lax.broadcasted_iota(jnp.int32, (LANES, local), 0)
    columns = jnp.zeros((LANES, local), jnp.float32)
    for k, tag in enumerate(tags):
        columns = jnp.where(row == k, tag, columns)
    columns = jnp.concatenate([columns, jnp.zeros((LANES, LANES - local), jnp.float32)], axis=1)
    out_ref[:, depth:] = columns.T[:local].astype(jnp.bfloat16)
    copies[3].wait()


def score_kernel(index_ref, a_ref, b_ref, *refs):
    *blocks, stats_ref, meta_ref, x_ref, tiles, logits, peak, sems = refs
    rows, depth = x_ref.shape[0], a_ref.shape[0]
    per_head = a_ref.shape[1] // TILE
    count = 2 * per_head
    copies = []
    for j in range(count):
        source = (a_ref, b_ref)[j // per_head].at[:, pl.ds(j % per_head * TILE, TILE)]
        copies.append(pltpu.make_async_copy(source, tiles.at[j], sems.at[j]))
        copies[j].start()
    peak[...] = jnp.full(peak.shape, -jnp.inf, jnp.float32)

    def take(some):
        for k in some:
            place = pl.multiple_of(index_ref[HEADER + k], blocks[k].shape[0])
            x_ref[pl.ds(place, blocks[k].shape[0]), :] = blocks[k][...]

    first, last = range(4), range(len(blocks) - 4, len(blocks))
    take(range(4, len(blocks) - 4))
    pl.when(index_ref[2] == 0)(lambda: take(first))
    pl.when(index_ref[2] != 0)(lambda: take(last))

    for j, copy in enumerate(copies):
        copy.wait()
        part = jnp.dot(x_ref[:, :depth], tiles[j], preferred_element_type=jnp.float32)
        logits[j] = part
        top = peak[...]
        for h in range(TILE // LANES):
            top = jnp.maximum(top, part[:, h * LANES : (h + 1) * LANES])
        peak[...] = top

    lane = lax.broadcasted_iota(jnp.int32, (1, LANES), 1).astype(jnp.float32)

    def read(tags, scales):
        weight = jnp.zeros(lane.shape, jnp.float32)
        for k, scale in scales:
            weight = jnp.where(lane == k, scale, weight)
        return tags * weight

    for r in range(rows // LANES):
        span = pl.ds(r * LANES, LANES)
        tags = x_ref[span, depth : depth + LANES].astype(jnp.float32)
        target = jnp.sum(read(tags, ((0, 65536.0), (1, 256.0), (2, 1.0))), axis=1, keepdims=True)
        top = peak[span, :]
        highest = jnp.max(top, axis=1, keepdims=True)
        scaled = jnp.zeros((LANES, LANES), jnp.float32)
        picked = jnp.zeros((LANES, LANES), jnp.float32)
        for j in range(count):
            for h in range(TILE // LANES):
                part = logits[j, span, h * LANES : (h + 1) * LANES]
                scaled += jnp.exp(part - highest)
                column = index_ref[j // per_head] + (j % per_head * TILE + h * LANES)
                picked += jnp.where(lane == target - column.astype(jnp.float32), part, 0.0)
        lse = jnp.max(top.T, axis=0, keepdims=True) + jnp.log(
            jnp.sum(scaled.T, axis=0, keepdims=True)
        )
        chosen = jnp.sum(picked.T, axis=0, keepdims=True)
        for k in range(stats_ref.shape[0]):
            stats_ref[k, :, r * LANES : (r + 1) * LANES] = lse
            stats_ref[k, :, rows + r * LANES : rows + (r + 1) * LANES] = chosen
        seq = jnp.sum(read(tags, ((3, 256.0), (4, 1.0))).T, axis=0, keepdims=True)
        parts = tags.T
        meta_ref[0:1, r * LANES : (r + 1) * LANES] = seq
        meta_ref[1:2, r * LANES : (r + 1) * LANES] = parts[5:6] + parts[6:7] + parts[7:8]


def merged(parts_ref):
    n, _, width = parts_ref.shape
    rows = width // 2
    lses = [parts_ref[k, :, :rows] for k in range(n)]
    highest = functools.reduce(jnp.maximum, lses)
    lse = highest + jnp.log(sum(jnp.exp(l - highest) for l in lses))
    return lse, sum(parts_ref[k, :, rows:] for k in range(n))


def merge_kernel(index_ref, parts_ref, meta_ref, out_ref, *, half):
    lse, picked = merged(parts_ref)
    rows = lse.shape[1]
    lane = lax.broadcasted_iota(jnp.int32, (1, rows), 1)
    span = rows // (2 * half)
    slot = lax.rem(lax.div(lane, span), half)
    mine = (slot == index_ref[5]) & (index_ref[2] == 0)
    picked = picked + jnp.where(mine, meta_ref[1:2, :], 0.0)
    seq = jnp.where(mine, meta_ref[0:1, :], 0.0)
    low = jnp.where(lane < rows // 2, seq, 0.0)
    high = jnp.where(lane < rows // 2, 0.0, seq)
    shift = index_ref[5] * span
    low = pltpu.roll(low, lax.rem(rows - shift, rows), 1)
    high = pltpu.roll(high, lax.rem(rows // 2 + rows - shift + span, rows), 1)
    ids = (low + high)[:, :LANES]
    for k in range(out_ref.shape[0]):
        out_ref[k, :, :rows] = lse
        out_ref[k, :, rows : 2 * rows] = picked
        out_ref[k, :, 2 * rows :] = ids


def held(z, c, nz):
    half = nz // 2
    return {(z - s if c == 0 else z + 1 + s) % nz for s in range(half)}


def finish_kernel(index_ref, parts_ref, own_ref, score_ref, *, nz, span):
    rows, count, half = (parts_ref.shape[2] - LANES) // 2, score_ref.shape[1], nz // 2
    lane = lax.broadcasted_iota(jnp.int32, (1, rows), 1)
    slot = lax.rem(lax.div(lane, span), half)

    def field(k, i):
        return parts_ref[k, :, i * rows : (i + 1) * rows]

    excesses, sums = [], None
    for low in (True, False):
        lses, picked = [], jnp.zeros((1, rows), jnp.float32)
        seq = jnp.zeros((1, rows), jnp.float32)
        for k in range(2 * nz):
            zs = [z for z in held(k // 2, k % 2, nz) if (z < half) == low]
            if not zs:
                continue
            here = functools.reduce(jnp.logical_or, [slot == z % half for z in zs])
            lses.append(jnp.where(here, field(k, 0), -jnp.inf))
            picked += jnp.where(here, field(k, 1), 0.0)
        for z in range(nz):
            if (z < half) == low:
                ids = jnp.concatenate([parts_ref[2 * z, :, 2 * rows :]] + [jnp.zeros((1, LANES), jnp.float32)] * (rows // LANES - 1), axis=1)
                even = jnp.where(lane < span, ids, 0.0)
                shift = z % half * span
                even = pltpu.roll(even, shift, 1) if shift else even
                odd = jnp.where(lane < span, 0.0, ids)
                seq += even + pltpu.roll(odd, rows // 2 - span + shift, 1)
        highest = functools.reduce(jnp.maximum, lses)
        lse = highest + jnp.log(sum(jnp.exp(l - highest) for l in lses))
        excess = lse - picked
        excesses.append(excess)
        ids = lax.broadcasted_iota(jnp.int32, (count, rows), 0).astype(jnp.float32)
        member = jnp.where(ids == seq, 1.0, 0.0).astype(jnp.bfloat16)
        high = excess.astype(jnp.bfloat16).astype(jnp.float32)
        middle = (excess - high).astype(jnp.bfloat16).astype(jnp.float32)
        pieces = [high, middle, excess - high - middle, jnp.ones_like(excess)]
        row = lax.broadcasted_iota(jnp.int32, (16, rows), 0)
        left = jnp.zeros((16, rows), jnp.float32)
        for i, piece in enumerate(pieces):
            left = jnp.where(row == i, piece, left)
        part = lax.dot_general(
            left.astype(jnp.bfloat16), member, (((1,), (1,)), ((), ())),
            preferred_element_type=jnp.float32,
        )
        sums = part if sums is None else sums + part
    score_ref[...] = (sums[0:1] + sums[1:2] + sums[2:3]) / sums[3:4]
    mine = jnp.where(index_ref[4] == 0, excesses[0], excesses[1])
    own_ref[...] = pltpu.roll(mine, lax.rem(rows - index_ref[3], rows), 1)[:, :LANES]


def on_device(states, head, targets, ref_loss, seq_ids):
    xl, z, c = (lax.axis_index(a) for a in TOK)
    nz = lax.axis_size("z")
    half = nz // 2
    local = states.shape[0]
    depth, width = head.shape
    tagged = pl.pallas_call(
        tag_kernel,
        out_shape=jax.ShapeDtypeStruct((local, depth + LANES), jnp.bfloat16),
        in_specs=[HBM] * 4,
        out_specs=VMEM,
        scratch_shapes=[
            pltpu.VMEM((1, local), jnp.int32),
            pltpu.VMEM((1, local), jnp.float32),
            pltpu.VMEM((1, local), jnp.int32),
            pltpu.SemaphoreType.DMA((4,)),
        ],
        compiler_params=pltpu.CompilerParams(
            vmem_limit_bytes=VMEM_BYTES - 3 * local * (depth + LANES)
        ),
        name="tag",
    )(states, targets[None], ref_loss[None], seq_ids[None])

    other_half = hop(tagged, "c", 1)

    def along(value, axis, first, second):
        n = lax.axis_size(axis)
        pairs = [(2 * i, (i + 1) % n * 2) for i in range(n)] if first else []
        pairs += [(2 * i + 1, (i - 1) % n * 2 + 1) for i in range(n)] if second else []
        axes = (axis, "c") if isinstance(axis, str) else (*axis, "c")
        return lax.ppermute(value, axes, pairs)

    near = [tagged, other_half]
    blocks, where = [], []
    for s in range(half + 1):
        if s > 0:
            for k in range(2):
                near[k] = along(near[k], "z", s < half, True)
        for k in range(2):
            far = along(near[k], X, s < half, s > 0)
            blocks += [near[k], far]
            where += [(s, 0, k), (s, 1, k)]
    partner_head = hop(head, "c", 1)

    block = lax.axis_index(("xh", "y")) * lax.axis_size(TOK) + (xl * nz + z) * 2
    steps, other, piece = jnp.asarray([(0, 0, 0)] * HEADER + where, jnp.int32).T
    k = lax.iota(jnp.int32, steps.shape[0])
    span = 2 * local
    slot = lax.rem(z + jnp.where(c == 0, nz - steps, steps), half)
    index = ((xl ^ other) * half + slot) * span + (c ^ piece) * local
    fixed = ((block + c) * width, (block + 1 - c) * width, c, (xl * half + z % half) * span + c * local, z // half, z % half)
    for i, value in enumerate(fixed):
        index = jnp.where(k == i, value, index)
    tokens = 2 * nz * local
    plane = lax.axis_size(PLANE)
    count = 2 * width // TILE
    stats, meta = pl.pallas_call(
        score_kernel,
        out_shape=(
            jax.ShapeDtypeStruct((plane, 1, 2 * tokens), jnp.float32),
            jax.ShapeDtypeStruct((2, tokens), jnp.float32),
        ),
        in_specs=[SMEM, HBM, HBM] + [VMEM] * len(blocks),
        out_specs=(VMEM, VMEM),
        scratch_shapes=[
            pltpu.VMEM((tokens, depth + LANES), jnp.bfloat16),
            pltpu.VMEM((count, depth, TILE), jnp.bfloat16),
            pltpu.VMEM((count, tokens, TILE), jnp.float32),
            pltpu.VMEM((tokens, LANES), jnp.float32),
            pltpu.SemaphoreType.DMA((count,)),
        ],
        compiler_params=pltpu.CompilerParams(vmem_limit_bytes=45 << 20),
        cost_estimate=pl.CostEstimate(
            flops=4 * tokens * depth * width, bytes_accessed=4 * depth * width, transcendentals=0
        ),
        name="score",
    )(index, head, partner_head, *blocks)
    stats = pl.pallas_call(
        functools.partial(merge_kernel, half=half),
        out_shape=jax.ShapeDtypeStruct((2 * nz, 1, 2 * tokens + LANES), jnp.float32),
        in_specs=[SMEM, VMEM, VMEM],
        out_specs=VMEM,
        compiler_params=pltpu.CompilerParams(vmem_limit_bytes=2 << 20),
        name="merge",
    )(index, exchange(stats, PLANE), meta)
    own, score = pl.pallas_call(
        functools.partial(finish_kernel, nz=nz, span=span),
        out_shape=(
            jax.ShapeDtypeStruct((1, LANES), jnp.float32),
            jax.ShapeDtypeStruct((1, tokens), jnp.float32),
        ),
        in_specs=[SMEM, VMEM],
        out_specs=(VMEM, VMEM),
        compiler_params=pltpu.CompilerParams(vmem_limit_bytes=8 << 20),
        name="finish",
    )(index, exchange(stats, ("z", "c")))
    return own[0, :local], score[0]


def solution(mesh):
    torus = Mesh(mesh.devices.reshape(2, 4, 2, 8, 2), BLK_TOK)
    return jax.shard_map(
        on_device,
        mesh=torus,
        in_specs=(P(TOK, None), P(None, BLK_TOK), P(TOK), P(TOK), P(TOK)),
        out_specs=(P(TOK), P()),
        check_vma=False,
    )
```

```python
import functools

import jax
import jax.numpy as jnp
from jax import lax
from jax.experimental import pallas as pl
from jax.experimental.pallas import tpu as pltpu
from jax.sharding import Mesh
from jax.sharding import PartitionSpec as P


TOK = ("xl", "z", "c")
BLK_TOK = ("xh", "y", "xl", "z", "c")
X = ("xh", "xl")
PLANE = ("xh", "xl", "y")
LANES = 128
TILE = 512
VMEM_BYTES = 67043328
HEADER = 6

VMEM = pl.BlockSpec(memory_space=pltpu.VMEM)
SMEM = pl.BlockSpec(memory_space=pltpu.SMEM)
HBM = pl.BlockSpec(memory_space=pltpu.HBM)


def hop(value, axis, step):
    n = lax.axis_size(axis)
    return lax.ppermute(value, axis, [(i, (i + step) % n) for i in range(n)])


def exchange(copies, axis):
    return lax.all_to_all(copies, axis, 0, 0, tiled=True)


def tag_kernel(states_in, targets_in, loss_in, seq_in, out_ref, targets_ref, loss_ref, seq_ref, sems):
    local, depth = states_in.shape
    pairs = (
        (targets_in, targets_ref),
        (loss_in, loss_ref),
        (seq_in, seq_ref),
        (states_in, out_ref.at[:, pl.ds(0, depth)]),
    )
    copies = [pltpu.make_async_copy(a, b, sems.at[k]) for k, (a, b) in enumerate(pairs)]
    for copy in copies:
        copy.start()
    for copy in copies[:3]:
        copy.wait()
    target, seq, loss = targets_ref[...], seq_ref[...], loss_ref[...]
    high = loss.astype(jnp.bfloat16).astype(jnp.float32)
    middle = (loss - high).astype(jnp.bfloat16).astype(jnp.float32)
    tags = [target >> 16, (target >> 8) & 255, target & 255, seq >> 8, seq & 255]
    tags = [t.astype(jnp.float32) for t in tags] + [high, middle, loss - high - middle]
    row = lax.broadcasted_iota(jnp.int32, (LANES, local), 0)
    columns = jnp.zeros((LANES, local), jnp.float32)
    for k, tag in enumerate(tags):
        columns = jnp.where(row == k, tag, columns)
    columns = jnp.concatenate([columns, jnp.zeros((LANES, LANES - local), jnp.float32)], axis=1)
    out_ref[:, depth:] = columns.T[:local].astype(jnp.bfloat16)
    copies[3].wait()


def score_kernel(index_ref, a_ref, b_ref, *refs):
    *blocks, stats_ref, meta_ref, x_ref, tiles, logits, peak, sems = refs
    rows, depth = x_ref.shape[0], a_ref.shape[0]
    per_head = a_ref.shape[1] // TILE
    count = 2 * per_head
    copies = []
    for j in range(count):
        source = (a_ref, b_ref)[j // per_head].at[:, pl.ds(j % per_head * TILE, TILE)]
        copies.append(pltpu.make_async_copy(source, tiles.at[j], sems.at[j]))
        copies[j].start()
    peak[...] = jnp.full(peak.shape, -jnp.inf, jnp.float32)
    for k, block in enumerate(blocks):
        place = pl.multiple_of(index_ref[HEADER + k], block.shape[0])
        x_ref[pl.ds(place, block.shape[0]), :] = block[...]

    for j, copy in enumerate(copies):
        copy.wait()
        part = jnp.dot(x_ref[:, :depth], tiles[j], preferred_element_type=jnp.float32)
        logits[j] = part
        top = peak[...]
        for h in range(TILE // LANES):
            top = jnp.maximum(top, part[:, h * LANES : (h + 1) * LANES])
        peak[...] = top

    lane = lax.broadcasted_iota(jnp.int32, (1, LANES), 1).astype(jnp.float32)

    def read(tags, scales):
        weight = jnp.zeros(lane.shape, jnp.float32)
        for k, scale in scales:
            weight = jnp.where(lane == k, scale, weight)
        return tags * weight

    for r in range(rows // LANES):
        span = pl.ds(r * LANES, LANES)
        tags = x_ref[span, depth : depth + LANES].astype(jnp.float32)
        target = jnp.sum(read(tags, ((0, 65536.0), (1, 256.0), (2, 1.0))), axis=1, keepdims=True)
        top = peak[span, :]
        highest = jnp.max(top, axis=1, keepdims=True)
        scaled = jnp.zeros((LANES, LANES), jnp.float32)
        picked = jnp.zeros((LANES, LANES), jnp.float32)
        for j in range(count):
            for h in range(TILE // LANES):
                part = logits[j, span, h * LANES : (h + 1) * LANES]
                scaled += jnp.exp(part - highest)
                column = index_ref[j // per_head] + (j % per_head * TILE + h * LANES)
                picked += jnp.where(lane == target - column.astype(jnp.float32), part, 0.0)
        lse = jnp.max(top.T, axis=0, keepdims=True) + jnp.log(
            jnp.sum(scaled.T, axis=0, keepdims=True)
        )
        chosen = jnp.sum(picked.T, axis=0, keepdims=True)
        for k in range(stats_ref.shape[0]):
            stats_ref[k, :, r * LANES : (r + 1) * LANES] = lse
            stats_ref[k, :, rows + r * LANES : rows + (r + 1) * LANES] = chosen
        seq = jnp.sum(read(tags, ((3, 256.0), (4, 1.0))).T, axis=0, keepdims=True)
        parts = tags.T
        meta_ref[0:1, r * LANES : (r + 1) * LANES] = seq
        meta_ref[1:2, r * LANES : (r + 1) * LANES] = parts[5:6] + parts[6:7] + parts[7:8]


def merged(parts_ref):
    n, _, width = parts_ref.shape
    rows = width // 2
    lses = [parts_ref[k, :, :rows] for k in range(n)]
    highest = functools.reduce(jnp.maximum, lses)
    lse = highest + jnp.log(sum(jnp.exp(l - highest) for l in lses))
    return lse, sum(parts_ref[k, :, rows:] for k in range(n))


def merge_kernel(index_ref, parts_ref, meta_ref, out_ref, *, half):
    lse, picked = merged(parts_ref)
    rows = lse.shape[1]
    lane = lax.broadcasted_iota(jnp.int32, (1, rows), 1)
    span = rows // (2 * half)
    slot = lax.rem(lax.div(lane, span), half)
    mine = (slot == index_ref[5]) & (index_ref[2] == 0)
    picked = picked + jnp.where(mine, meta_ref[1:2, :], 0.0)
    seq = jnp.where(mine, meta_ref[0:1, :], 0.0)
    low = jnp.where(lane < rows // 2, seq, 0.0)
    high = jnp.where(lane < rows // 2, 0.0, seq)
    shift = index_ref[5] * span
    low = pltpu.roll(low, lax.rem(rows - shift, rows), 1)
    high = pltpu.roll(high, lax.rem(rows // 2 + rows - shift + span, rows), 1)
    ids = (low + high)[:, :LANES]
    for k in range(out_ref.shape[0]):
        out_ref[k, :, :rows] = lse
        out_ref[k, :, rows : 2 * rows] = picked
        out_ref[k, :, 2 * rows :] = ids


def held(z, c, nz):
    half = nz // 2
    return {(z - s if c == 0 else z + 1 + s) % nz for s in range(half)}


def finish_kernel(index_ref, parts_ref, own_ref, score_ref, *, nz, span):
    rows, count, half = (parts_ref.shape[2] - LANES) // 2, score_ref.shape[1], nz // 2
    lane = lax.broadcasted_iota(jnp.int32, (1, rows), 1)
    slot = lax.rem(lax.div(lane, span), half)

    def field(k, i):
        return parts_ref[k, :, i * rows : (i + 1) * rows]

    excesses, sums = [], None
    for low in (True, False):
        lses, picked = [], jnp.zeros((1, rows), jnp.float32)
        seq = jnp.zeros((1, rows), jnp.float32)
        for k in range(2 * nz):
            zs = [z for z in held(k // 2, k % 2, nz) if (z < half) == low]
            if not zs:
                continue
            here = functools.reduce(jnp.logical_or, [slot == z % half for z in zs])
            lses.append(jnp.where(here, field(k, 0), -jnp.inf))
            picked += jnp.where(here, field(k, 1), 0.0)
        for z in range(nz):
            if (z < half) == low:
                ids = jnp.concatenate([parts_ref[2 * z, :, 2 * rows :]] + [jnp.zeros((1, LANES), jnp.float32)] * (rows // LANES - 1), axis=1)
                even = jnp.where(lane < span, ids, 0.0)
                shift = z % half * span
                even = pltpu.roll(even, shift, 1) if shift else even
                odd = jnp.where(lane < span, 0.0, ids)
                seq += even + pltpu.roll(odd, rows // 2 - span + shift, 1)
        highest = functools.reduce(jnp.maximum, lses)
        lse = highest + jnp.log(sum(jnp.exp(l - highest) for l in lses))
        excess = lse - picked
        excesses.append(excess)
        ids = lax.broadcasted_iota(jnp.int32, (count, rows), 0).astype(jnp.float32)
        member = jnp.where(ids == seq, 1.0, 0.0).astype(jnp.bfloat16)
        high = excess.astype(jnp.bfloat16).astype(jnp.float32)
        middle = (excess - high).astype(jnp.bfloat16).astype(jnp.float32)
        pieces = [high, middle, excess - high - middle, jnp.ones_like(excess)]
        row = lax.broadcasted_iota(jnp.int32, (16, rows), 0)
        left = jnp.zeros((16, rows), jnp.float32)
        for i, piece in enumerate(pieces):
            left = jnp.where(row == i, piece, left)
        part = lax.dot_general(
            left.astype(jnp.bfloat16), member, (((1,), (1,)), ((), ())),
            preferred_element_type=jnp.float32,
        )
        sums = part if sums is None else sums + part
    score_ref[...] = (sums[0:1] + sums[1:2] + sums[2:3]) / sums[3:4]
    mine = jnp.where(index_ref[4] == 0, excesses[0], excesses[1])
    own_ref[...] = pltpu.roll(mine, lax.rem(rows - index_ref[3], rows), 1)[:, :LANES]


def on_device(states, head, targets, ref_loss, seq_ids):
    xl, z, c = (lax.axis_index(a) for a in TOK)
    nz = lax.axis_size("z")
    half = nz // 2
    local = states.shape[0]
    depth, width = head.shape
    tagged = pl.pallas_call(
        tag_kernel,
        out_shape=jax.ShapeDtypeStruct((local, depth + LANES), jnp.bfloat16),
        in_specs=[HBM] * 4,
        out_specs=VMEM,
        scratch_shapes=[
            pltpu.VMEM((1, local), jnp.int32),
            pltpu.VMEM((1, local), jnp.float32),
            pltpu.VMEM((1, local), jnp.int32),
            pltpu.SemaphoreType.DMA((4,)),
        ],
        compiler_params=pltpu.CompilerParams(
            vmem_limit_bytes=VMEM_BYTES - 3 * local * (depth + LANES)
        ),
        name="tag",
    )(states, targets[None], ref_loss[None], seq_ids[None])

    other_half = hop(tagged, "c", 1)

    def along(value, axis, first, second):
        n = lax.axis_size(axis)
        pairs = [(2 * i, (i + 1) % n * 2) for i in range(n)] if first else []
        pairs += [(2 * i + 1, (i - 1) % n * 2 + 1) for i in range(n)] if second else []
        axes = (axis, "c") if isinstance(axis, str) else (*axis, "c")
        return lax.ppermute(value, axes, pairs)

    start = near = [tagged, other_half]
    blocks, where = [], []
    for s in range(1, half + 1):
        moved = []
        for k in range(2):
            moved.append(along(near[k], "z", s < half, True))
        near = moved
        for k in range(2):
            kept = jnp.where(c == 0, start[k], near[k]) if s == half else near[k]
            far = along(kept, X, True, True)
            blocks += [kept, far]
            where += [(s, 0, k), (s, 1, k)]
    partner_head = hop(head, "c", 1)

    block = lax.axis_index(("xh", "y")) * lax.axis_size(TOK) + (xl * nz + z) * 2
    steps, other, piece = jnp.asarray([(0, 0, 0)] * HEADER + where, jnp.int32).T
    k = lax.iota(jnp.int32, steps.shape[0])
    span = 2 * local
    slot = lax.rem(z + jnp.where(c == 0, nz - steps, steps), half)
    index = ((xl ^ other) * half + slot) * span + (c ^ piece) * local
    fixed = ((block + c) * width, (block + 1 - c) * width, c, (xl * half + z % half) * span + c * local, z // half, z % half)
    for i, value in enumerate(fixed):
        index = jnp.where(k == i, value, index)
    tokens = 2 * nz * local
    plane = lax.axis_size(PLANE)
    count = 2 * width // TILE
    stats, meta = pl.pallas_call(
        score_kernel,
        out_shape=(
            jax.ShapeDtypeStruct((plane, 1, 2 * tokens), jnp.float32),
            jax.ShapeDtypeStruct((2, tokens), jnp.float32),
        ),
        in_specs=[SMEM, HBM, HBM] + [VMEM] * len(blocks),
        out_specs=(VMEM, VMEM),
        scratch_shapes=[
            pltpu.VMEM((tokens, depth + LANES), jnp.bfloat16),
            pltpu.VMEM((count, depth, TILE), jnp.bfloat16),
            pltpu.VMEM((count, tokens, TILE), jnp.float32),
            pltpu.VMEM((tokens, LANES), jnp.float32),
            pltpu.SemaphoreType.DMA((count,)),
        ],
        compiler_params=pltpu.CompilerParams(vmem_limit_bytes=45 << 20),
        cost_estimate=pl.CostEstimate(
            flops=4 * tokens * depth * width, bytes_accessed=4 * depth * width, transcendentals=0
        ),
        name="score",
    )(index, head, partner_head, *blocks)
    stats = pl.pallas_call(
        functools.partial(merge_kernel, half=half),
        out_shape=jax.ShapeDtypeStruct((2 * nz, 1, 2 * tokens + LANES), jnp.float32),
        in_specs=[SMEM, VMEM, VMEM],
        out_specs=VMEM,
        compiler_params=pltpu.CompilerParams(vmem_limit_bytes=2 << 20),
        name="merge",
    )(index, exchange(stats, PLANE), meta)
    own, score = pl.pallas_call(
        functools.partial(finish_kernel, nz=nz, span=span),
        out_shape=(
            jax.ShapeDtypeStruct((1, LANES), jnp.float32),
            jax.ShapeDtypeStruct((1, tokens), jnp.float32),
        ),
        in_specs=[SMEM, VMEM],
        out_specs=(VMEM, VMEM),
        compiler_params=pltpu.CompilerParams(vmem_limit_bytes=8 << 20),
        name="finish",
    )(index, exchange(stats, ("z", "c")))
    return own[0, :local], score[0]


def solution(mesh):
    torus = Mesh(mesh.devices.reshape(2, 4, 2, 8, 2), BLK_TOK)
    return jax.shard_map(
        on_device,
        mesh=torus,
        in_specs=(P(TOK, None), P(None, BLK_TOK), P(TOK), P(TOK), P(TOK)),
        out_specs=(P(TOK), P()),
        check_vma=False,
    )
```

```python
import functools

import jax
import jax.numpy as jnp
from jax import lax
from jax.experimental import pallas as pl
from jax.experimental.pallas import tpu as pltpu
from jax.sharding import Mesh
from jax.sharding import PartitionSpec as P


TOK = ("xl", "z", "c")
BLK_TOK = ("xh", "y", "xl", "z", "c")
X = ("xh", "xl")
PLANE = ("xh", "xl", "y")
LANES = 128
TILE = 512
VMEM_BYTES = 67043328
HEADER = 6

VMEM = pl.BlockSpec(memory_space=pltpu.VMEM)
SMEM = pl.BlockSpec(memory_space=pltpu.SMEM)
HBM = pl.BlockSpec(memory_space=pltpu.HBM)


def hop(value, axis, step):
    n = lax.axis_size(axis)
    return lax.ppermute(value, axis, [(i, (i + step) % n) for i in range(n)])


def exchange(copies, axis):
    return lax.all_to_all(copies, axis, 0, 0, tiled=True)


def tag_kernel(states_in, targets_in, loss_in, seq_in, out_ref, targets_ref, loss_ref, seq_ref, sems):
    local, depth = states_in.shape
    pairs = (
        (targets_in, targets_ref),
        (loss_in, loss_ref),
        (seq_in, seq_ref),
        (states_in, out_ref.at[:, pl.ds(0, depth)]),
    )
    copies = [pltpu.make_async_copy(a, b, sems.at[k]) for k, (a, b) in enumerate(pairs)]
    for copy in copies:
        copy.start()
    for copy in copies[:3]:
        copy.wait()
    target, seq, loss = targets_ref[...], seq_ref[...], loss_ref[...]
    high = loss.astype(jnp.bfloat16).astype(jnp.float32)
    middle = (loss - high).astype(jnp.bfloat16).astype(jnp.float32)
    tags = [target >> 16, (target >> 8) & 255, target & 255, seq >> 8, seq & 255]
    tags = [t.astype(jnp.float32) for t in tags] + [high, middle, loss - high - middle]
    row = lax.broadcasted_iota(jnp.int32, (LANES, local), 0)
    columns = jnp.zeros((LANES, local), jnp.float32)
    for k, tag in enumerate(tags):
        columns = jnp.where(row == k, tag, columns)
    columns = jnp.concatenate([columns, jnp.zeros((LANES, LANES - local), jnp.float32)], axis=1)
    out_ref[:, depth:] = columns.T[:local].astype(jnp.bfloat16)
    copies[3].wait()


def score_kernel(index_ref, a_ref, b_ref, *refs):
    *blocks, stats_ref, meta_ref, x_ref, tiles, logits, peak, sems = refs
    rows, depth = x_ref.shape[0], a_ref.shape[0]
    per_head = a_ref.shape[1] // TILE
    count = 2 * per_head
    copies = []
    for j in range(count):
        source = (a_ref, b_ref)[j // per_head].at[:, pl.ds(j % per_head * TILE, TILE)]
        copies.append(pltpu.make_async_copy(source, tiles.at[j], sems.at[j]))
        copies[j].start()
    peak[...] = jnp.full(peak.shape, -jnp.inf, jnp.float32)
    for k, block in enumerate(blocks):
        place = pl.multiple_of(index_ref[HEADER + k], block.shape[0])
        x_ref[pl.ds(place, block.shape[0]), :] = block[...]

    for j, copy in enumerate(copies):
        copy.wait()
        part = jnp.dot(x_ref[:, :depth], tiles[j], preferred_element_type=jnp.float32)
        logits[j] = part
        top = peak[...]
        for h in range(TILE // LANES):
            top = jnp.maximum(top, part[:, h * LANES : (h + 1) * LANES])
        peak[...] = top

    lane = lax.broadcasted_iota(jnp.int32, (1, LANES), 1).astype(jnp.float32)

    def read(tags, scales):
        weight = jnp.zeros(lane.shape, jnp.float32)
        for k, scale in scales:
            weight = jnp.where(lane == k, scale, weight)
        return tags * weight

    for r in range(rows // LANES):
        span = pl.ds(r * LANES, LANES)
        tags = x_ref[span, depth : depth + LANES].astype(jnp.float32)
        target = jnp.sum(read(tags, ((0, 65536.0), (1, 256.0), (2, 1.0))), axis=1, keepdims=True)
        top = peak[span, :]
        highest = jnp.max(top, axis=1, keepdims=True)
        scaled = jnp.zeros((LANES, LANES), jnp.float32)
        picked = jnp.zeros((LANES, LANES), jnp.float32)
        for j in range(count):
            for h in range(TILE // LANES):
                part = logits[j, span, h * LANES : (h + 1) * LANES]
                scaled += jnp.exp(part - highest)
                column = index_ref[j // per_head] + (j % per_head * TILE + h * LANES)
                picked += jnp.where(lane == target - column.astype(jnp.float32), part, 0.0)
        lse = jnp.max(top.T, axis=0, keepdims=True) + jnp.log(
            jnp.sum(scaled.T, axis=0, keepdims=True)
        )
        chosen = jnp.sum(picked.T, axis=0, keepdims=True)
        for k in range(stats_ref.shape[0]):
            stats_ref[k, :, r * LANES : (r + 1) * LANES] = lse
            stats_ref[k, :, rows + r * LANES : rows + (r + 1) * LANES] = chosen
        seq = jnp.sum(read(tags, ((3, 256.0), (4, 1.0))).T, axis=0, keepdims=True)
        parts = tags.T
        meta_ref[0:1, r * LANES : (r + 1) * LANES] = seq
        meta_ref[1:2, r * LANES : (r + 1) * LANES] = parts[5:6] + parts[6:7] + parts[7:8]


def merged(parts_ref):
    n, _, width = parts_ref.shape
    rows = width // 2
    lses = [parts_ref[k, :, :rows] for k in range(n)]
    highest = functools.reduce(jnp.maximum, lses)
    lse = highest + jnp.log(sum(jnp.exp(l - highest) for l in lses))
    return lse, sum(parts_ref[k, :, rows:] for k in range(n))


def merge_kernel(index_ref, parts_ref, meta_ref, out_ref, *, half):
    lse, picked = merged(parts_ref)
    rows = lse.shape[1]
    lane = lax.broadcasted_iota(jnp.int32, (1, rows), 1)
    span = rows // (2 * half)
    slot = lax.rem(lax.div(lane, span), half)
    mine = (slot == index_ref[5]) & (index_ref[2] == 0)
    picked = picked + jnp.where(mine, meta_ref[1:2, :], 0.0)
    seq = jnp.where(mine, meta_ref[0:1, :], 0.0)
    low = jnp.where(lane < rows // 2, seq, 0.0)
    high = jnp.where(lane < rows // 2, 0.0, seq)
    shift = index_ref[5] * span
    low = pltpu.roll(low, lax.rem(rows - shift, rows), 1)
    high = pltpu.roll(high, lax.rem(rows // 2 + rows - shift + span, rows), 1)
    ids = (low + high)[:, :LANES]
    for k in range(out_ref.shape[0]):
        out_ref[k, :, :rows] = lse
        out_ref[k, :, rows : 2 * rows] = picked
        out_ref[k, :, 2 * rows :] = ids


def held(z, c, nz):
    half = nz // 2
    return {(z - s if c == 0 else z + 1 + s) % nz for s in range(half)}


def finish_kernel(index_ref, parts_ref, own_ref, score_ref, *, nz, span):
    rows, count, half = (parts_ref.shape[2] - LANES) // 2, score_ref.shape[1], nz // 2
    lane = lax.broadcasted_iota(jnp.int32, (1, rows), 1)
    slot = lax.rem(lax.div(lane, span), half)

    def field(k, i):
        return parts_ref[k, :, i * rows : (i + 1) * rows]

    excesses, sums = [], None
    for low in (True, False):
        lses, picked = [], jnp.zeros((1, rows), jnp.float32)
        seq = jnp.zeros((1, rows), jnp.float32)
        for k in range(2 * nz):
            zs = [z for z in held(k // 2, k % 2, nz) if (z < half) == low]
            if not zs:
                continue
            here = functools.reduce(jnp.logical_or, [slot == z % half for z in zs])
            lses.append(jnp.where(here, field(k, 0), -jnp.inf))
            picked += jnp.where(here, field(k, 1), 0.0)
        for z in range(nz):
            if (z < half) == low:
                ids = jnp.concatenate([parts_ref[2 * z, :, 2 * rows :]] + [jnp.zeros((1, LANES), jnp.float32)] * (rows // LANES - 1), axis=1)
                even = jnp.where(lane < span, ids, 0.0)
                shift = z % half * span
                even = pltpu.roll(even, shift, 1) if shift else even
                odd = jnp.where(lane < span, 0.0, ids)
                seq += even + pltpu.roll(odd, rows // 2 - span + shift, 1)
        highest = functools.reduce(jnp.maximum, lses)
        lse = highest + jnp.log(sum(jnp.exp(l - highest) for l in lses))
        excess = lse - picked
        excesses.append(excess)
        ids = lax.broadcasted_iota(jnp.int32, (count, rows), 0).astype(jnp.float32)
        member = jnp.where(ids == seq, 1.0, 0.0).astype(jnp.bfloat16)
        high = excess.astype(jnp.bfloat16).astype(jnp.float32)
        middle = (excess - high).astype(jnp.bfloat16).astype(jnp.float32)
        pieces = [high, middle, excess - high - middle, jnp.ones_like(excess)]
        row = lax.broadcasted_iota(jnp.int32, (16, rows), 0)
        left = jnp.zeros((16, rows), jnp.float32)
        for i, piece in enumerate(pieces):
            left = jnp.where(row == i, piece, left)
        part = lax.dot_general(
            left.astype(jnp.bfloat16), member, (((1,), (1,)), ((), ())),
            preferred_element_type=jnp.float32,
        )
        sums = part if sums is None else sums + part
    score_ref[...] = (sums[0:1] + sums[1:2] + sums[2:3]) / sums[3:4]
    mine = jnp.where(index_ref[4] == 0, excesses[0], excesses[1])
    own_ref[...] = pltpu.roll(mine, lax.rem(rows - index_ref[3], rows), 1)[:, : own_ref.shape[1]]


def on_device(states, head, targets, ref_loss, seq_ids):
    xl, z, c = (lax.axis_index(a) for a in TOK)
    nz = lax.axis_size("z")
    half = nz // 2
    local = states.shape[0]
    depth, width = head.shape
    tagged = pl.pallas_call(
        tag_kernel,
        out_shape=jax.ShapeDtypeStruct((local, depth + LANES), jnp.bfloat16),
        in_specs=[HBM] * 4,
        out_specs=VMEM,
        scratch_shapes=[
            pltpu.VMEM((1, local), jnp.int32),
            pltpu.VMEM((1, local), jnp.float32),
            pltpu.VMEM((1, local), jnp.int32),
            pltpu.SemaphoreType.DMA((4,)),
        ],
        compiler_params=pltpu.CompilerParams(
            vmem_limit_bytes=VMEM_BYTES - 3 * local * (depth + LANES)
        ),
        name="tag",
    )(states, targets[None], ref_loss[None], seq_ids[None])

    other_half = hop(tagged, "c", 1)

    def along(value, axis, first, second):
        n = lax.axis_size(axis)
        pairs = [(2 * i, (i + 1) % n * 2) for i in range(n)] if first else []
        pairs += [(2 * i + 1, (i - 1) % n * 2 + 1) for i in range(n)] if second else []
        axes = (axis, "c") if isinstance(axis, str) else (*axis, "c")
        return lax.ppermute(value, axes, pairs)

    start = near = [tagged, other_half]
    blocks, where = [], []
    for s in range(1, half + 1):
        moved = []
        for k in range(2):
            moved.append(along(near[k], "z", s < half, True))
        near = moved
        for k in range(2):
            kept = jnp.where(c == 0, start[k], near[k]) if s == half else near[k]
            far = along(kept, X, True, True)
            blocks += [kept, far]
            where += [(s, 0, k), (s, 1, k)]
    partner_head = hop(head, "c", 1)

    block = lax.axis_index(("xh", "y")) * lax.axis_size(TOK) + (xl * nz + z) * 2
    steps, other, piece = jnp.asarray([(0, 0, 0)] * HEADER + where, jnp.int32).T
    k = lax.iota(jnp.int32, steps.shape[0])
    span = 2 * local
    slot = lax.rem(z + jnp.where(c == 0, nz - steps, steps), half)
    index = ((xl ^ other) * half + slot) * span + (c ^ piece) * local
    fixed = ((block + c) * width, (block + 1 - c) * width, c, (xl * half + z % half) * span + c * local, z // half, z % half)
    for i, value in enumerate(fixed):
        index = jnp.where(k == i, value, index)
    tokens = 2 * nz * local
    plane = lax.axis_size(PLANE)
    count = 2 * width // TILE
    stats, meta = pl.pallas_call(
        score_kernel,
        out_shape=(
            jax.ShapeDtypeStruct((plane, 1, 2 * tokens), jnp.float32),
            jax.ShapeDtypeStruct((2, tokens), jnp.float32),
        ),
        in_specs=[SMEM, HBM, HBM] + [VMEM] * len(blocks),
        out_specs=(VMEM, VMEM),
        scratch_shapes=[
            pltpu.VMEM((tokens, depth + LANES), jnp.bfloat16),
            pltpu.VMEM((count, depth, TILE), jnp.bfloat16),
            pltpu.VMEM((count, tokens, TILE), jnp.float32),
            pltpu.VMEM((tokens, LANES), jnp.float32),
            pltpu.SemaphoreType.DMA((count,)),
        ],
        compiler_params=pltpu.CompilerParams(vmem_limit_bytes=45 << 20),
        cost_estimate=pl.CostEstimate(
            flops=4 * tokens * depth * width, bytes_accessed=4 * depth * width, transcendentals=0
        ),
        name="score",
    )(index, head, partner_head, *blocks)
    stats = pl.pallas_call(
        functools.partial(merge_kernel, half=half),
        out_shape=jax.ShapeDtypeStruct((2 * nz, 1, 2 * tokens + LANES), jnp.float32),
        in_specs=[SMEM, VMEM, VMEM],
        out_specs=VMEM,
        compiler_params=pltpu.CompilerParams(vmem_limit_bytes=2 << 20),
        name="merge",
    )(index, exchange(stats, PLANE), meta)
    own, score = pl.pallas_call(
        functools.partial(finish_kernel, nz=nz, span=span),
        out_shape=(
            jax.ShapeDtypeStruct((1, local), jnp.float32),
            jax.ShapeDtypeStruct((1, tokens), jnp.float32),
        ),
        in_specs=[SMEM, VMEM],
        out_specs=(VMEM, VMEM),
        compiler_params=pltpu.CompilerParams(vmem_limit_bytes=8 << 20),
        name="finish",
    )(index, exchange(stats, ("z", "c")))
    return own[0], score[0]


def solution(mesh):
    torus = Mesh(mesh.devices.reshape(2, 4, 2, 8, 2), BLK_TOK)
    return jax.shard_map(
        on_device,
        mesh=torus,
        in_specs=(P(TOK, None), P(None, BLK_TOK), P(TOK), P(TOK), P(TOK)),
        out_specs=(P(TOK), P()),
        check_vma=False,
    )
```
